128 devices in a mesh: dp: 32 (over z, x, core), rep: 4 (over y).
Axes of the slice: x: 4, y: 4, z: 4, core: 2. Of those that a mesh axis runs over, the one named last changes fastest.
Arguments:
- token_inputs: bfloat16 [65536, 2048], P(('dp', 'rep')), may hold values from -12 to 12
- cotangent: bfloat16 [65536, 2048], P(('dp', 'rep')), may hold values from -24 to 24
- gate_preact: bfloat16 [65536, 768], P(('dp', 'rep')), may hold values from -6 to 6
- up_preact: bfloat16 [65536, 768], P(('dp', 'rep')), may hold values from -6 to 6
- down_weight: bfloat16 [2, 768, 2048], P(None, None, 'dp'), may hold values from -0.21875 to 0.21875
- block_expert: int32 [512], P(('dp', 'rep')), may hold values from 0 to 1
- block_count: int32 [512], P(('dp', 'rep')), may hold values from 1 to 128, as said below
Outputs:
- update: bfloat16 [2, 3, 768, 2048], P(None, None, None, 'dp')
The draws below stay inside these ranges and needn't reach their ends.
Inputs may be any that keep to these rules, and one draw needn't show every extreme that they name: `block_count`: live rows of a block, at most 128; in every draw some block is full.
All inputs are finite; a program needn't handle non-finite values.
Results may differ from the reference program's by a relative error of at most 0.02.
Values may be sent and summed in bfloat16 or wider, within the bound.
No kernel may reach another device: no remote copies, remote signals or barrier semaphores. Data moves between devices by JAX's collectives and lax.ppermute only.
A program may use at most 128 MiB of HBM per device.

```python
import jax
import jax.numpy as jnp
from jax import lax

D = 2048
F = 768
EXPERTS = 2
BLOCK = 128
BLK = 4
ITERS = 2
ROWS = 65536
BLOCKS_ALL = 512
N_DP = 32
N_REP = 4


def draw_block_count(key, part):
    counts = jax.random.randint(key, (BLOCKS_ALL,), max(1, BLOCK // 4), BLOCK + 1, dtype=jnp.int32)
    chosen = jax.random.randint(jax.random.fold_in(key, 7), (), 0, BLOCKS_ALL, dtype=jnp.int32)
    return jnp.where(jnp.arange(BLOCKS_ALL, dtype=jnp.int32) == chosen, jnp.int32(BLOCK), counts)


def draw_token_inputs(key, part):
    column = jnp.arange(D, dtype=jnp.float32) / jnp.float32(max(D - 1, 1))
    ratio = 2.5
    base = jnp.clip(jax.random.normal(key, (ROWS, D), jnp.float32), -6.0, 6.0)
    scale = jnp.exp(jnp.log(jnp.float32(ratio)) * (column - 0.5))
    return (base * scale[None, :]).astype(jnp.bfloat16)


def plant(values, own_key, smallest, top_value):
    spot = [jax.random.randint(jax.random.fold_in(own_key, axis), (), 0, length) for axis, length in enumerate(values.shape)]
    longest = values.shape.index(max(values.shape))
    neighbour = spot[:longest] + [(spot[longest] + 1) % values.shape[longest]] + spot[longest + 1:]
    return values.at[tuple(spot)].set(smallest).at[tuple(neighbour)].set(top_value)


def spiked(values, own_key, source, target, shards_of, factor):
    def block_of(dim):
        return (jnp.arange(values.shape[dim]) // (values.shape[dim] // shards_of)).reshape((-1,) + (1,) * (values.ndim - 1 - dim))

    first = jax.random.permutation(own_key, shards_of)[block_of(target)]
    far = (block_of(target) + shards_of // 2) % shards_of
    return jnp.where((block_of(source) == first) | (block_of(source) == far), factor * values, values)


def level_of(stream_key, extent, shards, low, high):
    factor_of, own = 1.0, jax.random.fold_in(stream_key, 6)
    for position, blocks in shards:
        draws = jnp.exp(jax.random.uniform(jax.random.fold_in(own, position), (blocks,), jnp.float32, low / len(shards), high / len(shards)))
        factor_of = factor_of * jnp.repeat(draws, extent[position] // blocks).reshape([-1 if axis == position else 1 for axis in range(len(extent))])
    return factor_of


def normal_values(rng, dims, scale, most, pieces=(), kind=jnp.bfloat16):
    values = scale * jax.random.normal(rng, dims, jnp.float32)
    if pieces:
        values = values * level_of(rng, dims, pieces, -0.22, 0.18)
    return jnp.clip(values, -most, most).astype(kind)


def noise_with(key, extent, deviation, bound, pieces, heavy, held_as=jnp.bfloat16):
    drawn = deviation * jax.random.normal(key, extent, jnp.float32)
    if pieces:
        drawn = drawn * level_of(key, extent, pieces, -0.22, 0.18)
    return jnp.clip(spiked(drawn, jax.random.fold_in(key, 3), *heavy), -bound, bound).astype(held_as)


def setup_inputs(seed: int = 0) -> dict:
    key_list = jax.random.split(jax.random.key(seed), 8)
    token_inputs = draw_token_inputs(jax.random.fold_in(key_list[7], 71), 0)
    cotangent = noise_with(key_list[1], (ROWS, D), 1.0, 24.0, ((0, 128),), (0, 1, 128, 5.5))
    gate_preact = normal_values(key_list[2], (ROWS, F), 1.0, 6.0, ((0, 128),))
    up_preact = normal_values(key_list[3], (ROWS, F), 1.0, 6.0, ((0, 128),))
    down_weight = normal_values(key_list[4], (EXPERTS, F, D), F ** -0.5, 0.21875, ((2, 32),))
    block_expert = plant(jax.random.randint(key_list[5], (BLOCKS_ALL,), 0, EXPERTS), jax.random.fold_in(key_list[5], 1), 0, EXPERTS - 1).astype(jnp.int32)
    block_count = draw_block_count(jax.random.fold_in(key_list[7], 71), 0)
    return dict(token_inputs=token_inputs, cotangent=cotangent, gate_preact=gate_preact, up_preact=up_preact, down_weight=down_weight, block_expert=block_expert, block_count=block_count)


ns_first = 3.4445
ns_second = -4.775
ns_third = 2.0315
norm_eps = 1e-07

def device_partial(inputs, cotangent, gate_preact, up_preact, down_weight, experts, counts):
    blocks = counts.shape[0]
    width = inputs.shape[1]
    hidden_width = gate_preact.shape[1]
    inputs = inputs.reshape(blocks, BLOCK, width)
    cotangent = cotangent.reshape(blocks, BLOCK, width)
    gate = gate_preact.reshape(blocks, BLOCK, hidden_width).astype(jnp.float32)
    upper = up_preact.reshape(blocks, BLOCK, hidden_width).astype(jnp.float32)
    live_rows = jnp.arange(BLOCK, dtype=jnp.int32)[None, :] < counts[:, None]
    masked = jnp.where(live_rows[:, :, None], cotangent, jnp.zeros_like(cotangent))
    sigmoid_gate = jax.nn.sigmoid(gate)
    hidden = (gate * sigmoid_gate * upper).astype(jnp.bfloat16)
    chosen = jnp.take(down_weight, experts, axis=0)
    back = jnp.einsum('brd,bfd->brf', masked.astype(jnp.float32), chosen.astype(jnp.float32))
    grad_gate = (back * upper * sigmoid_gate * (1.0 + gate * (1.0 - sigmoid_gate))).astype(jnp.bfloat16)
    grad_up = (back * gate * sigmoid_gate).astype(jnp.bfloat16)
    left = jnp.stack([grad_gate, grad_up, hidden], 1).astype(jnp.float32)
    right = jnp.stack([inputs, inputs, masked], 1).astype(jnp.float32)
    per_block = jnp.einsum('bmrf,bmrd->bmfd', left, right)
    onehot = (experts[:, None] == jnp.arange(EXPERTS, dtype=jnp.int32)[None, :]).astype(jnp.float32)
    partial_value = jnp.einsum('be,bmfd->emfd', onehot, per_block, precision=lax.Precision.HIGHEST)
    return partial_value.astype(jnp.bfloat16)

def reference(token_inputs, cotangent, gate_preact, up_preact, down_weight, block_expert, block_count):
    devices_all = N_DP * N_REP
    rows_dev = BLK * BLOCK

    def add_device(total, index):
        first = (index * rows_dev).astype(jnp.int32)
        first_block = (index * BLK).astype(jnp.int32)
        partial_value = device_partial(lax.dynamic_slice_in_dim(token_inputs, first, rows_dev, 0), lax.dynamic_slice_in_dim(cotangent, first, rows_dev, 0), lax.dynamic_slice_in_dim(gate_preact, first, rows_dev, 0), lax.dynamic_slice_in_dim(up_preact, first, rows_dev, 0), down_weight, lax.dynamic_slice_in_dim(block_expert, first_block, BLK, 0), lax.dynamic_slice_in_dim(block_count, first_block, BLK, 0))
        return (total + partial_value.astype(jnp.float32), None)
    start_total = jnp.zeros((EXPERTS, 3, F, D), jnp.float32)
    grad, unused = lax.scan(add_device, start_total, jnp.arange(devices_all, dtype=jnp.int32))
    squares = lax.optimization_barrier(jnp.sum(grad * grad, axis=(2, 3)))
    current = (grad / (jnp.sqrt(squares) + norm_eps)[:, :, None, None]).astype(jnp.bfloat16)
    column_width = D // N_DP
    result = None
    for sweep in range(ITERS):
        as_float = current.astype(jnp.float32)
        split = as_float.reshape(EXPERTS, 3, F, N_DP, column_width)

        def add_columns(total, index):
            block_cols = lax.dynamic_index_in_dim(split, index, 3, False)
            term = jnp.einsum('emfd,emgd->emfg', block_cols, block_cols).astype(jnp.bfloat16)
            return (total + lax.optimization_barrier(term).astype(jnp.float32), None)
        gram, unused = lax.scan(add_columns, jnp.zeros((EXPERTS, 3, F, F), jnp.float32), jnp.arange(N_DP, dtype=jnp.int32))
        gram_half = gram.astype(jnp.bfloat16).astype(jnp.float32)
        squared = jnp.einsum('emfg,emgh->emfh', gram_half, gram_half)
        poly = (ns_second * gram + ns_third * squared).astype(jnp.bfloat16)
        newer = ns_first * as_float + jnp.einsum('emfg,emgd->emfd', poly.astype(jnp.float32), as_float)
        if sweep + 1 < ITERS:
            current = newer.astype(jnp.bfloat16)
        else:
            result = (jnp.sqrt(jnp.float32(D)) * newer).astype(jnp.bfloat16)
    return result
```

```python
import jax
import jax.numpy as jnp
from jax import lax
from jax.experimental import pallas as pl
from jax.experimental.pallas import tpu as pltpu
from jax.sharding import Mesh
from jax.sharding import PartitionSpec as P

DP = ("dp_0", "dp_1", "dp_2")
DP_REP = ("dp_0", "dp_1", "dp_2", "rep")

ns_first = 3.4445
ns_second = -4.775
ns_third = 2.0315
norm_eps = 1e-07

F = 768
D = 2048
BLOCK = 128
BLK = 4
HALF = D // 2
TILE = 512
RING = 4
CHUNK = F // RING
PIECE = CHUNK // RING
COLS = D // 16
SHIFTS = (1, 3, 2)
f32 = jnp.float32
bf16 = jnp.bfloat16


def shift(value, axis, by):
    return lax.ppermute(value, axis, [(i, (i + by) % RING) for i in range(RING)])


def swap(value):
    return lax.ppermute(value, "dp_2", [(0, 1), (1, 0)])


def row_mask(info, block, rows):
    limit = jnp.where(info[16 + block] == info[2], info[8 + block], 0)
    place = lax.broadcasted_iota(jnp.int32, (rows, F), 0)
    return place < limit


def hidden_kernel(info, gate_a, up_a, gate_b, up_b, cot_a, cot_b, *rest):
    outs, (left, acc) = rest[:8], rest[8:]
    step = pl.program_id(0)

    @pl.when(step == 0)
    def _():
        for block in range(2 * BLK):
            gate_ref, up_ref = (gate_a, up_a) if block < BLK else (gate_b, up_b)
            rows = pl.ds((block % BLK) * BLOCK, BLOCK)
            gate = gate_ref[rows, :].astype(f32)
            up = up_ref[rows, :].astype(f32)
            hidden = gate * jax.nn.sigmoid(gate) * up
            hidden = jnp.where(row_mask(info, block, BLOCK), hidden, 0.0)
            left[:, pl.ds(block * BLOCK, BLOCK)] = hidden.T.astype(bf16)

    rows = BLK * BLOCK
    acc[...] = jnp.dot(left[:, :rows], cot_a[...], preferred_element_type=f32) + jnp.dot(
        left[:, rows:], cot_b[...], preferred_element_type=f32
    )
    for half in range(2):

        @pl.when(step // 2 == half)
        def _(half=half):
            for s in range(RING):
                chunk = (info[half] + s) % RING
                outs[half * RING + s][0] = acc[pl.ds(chunk * CHUNK, CHUNK), :].astype(bf16)


def grads_kernel(info, gate_a, up_a, gate_b, up_b, cot_a, cot_b, tok_a, tok_b, *rest):
    weights, outs, (whole, back, left, acc) = rest[:8], rest[8:16], rest[16:]
    step = pl.program_id(0)
    rows = BLK * BLOCK

    @pl.when(step == 0)
    def _():
        for half in range(2):
            for t in range(RING):
                for s in range(RING):
                    near = (info[half] - s) % RING
                    far = (info[1 - half] - t) % RING
                    z, x = (near, far) if half == 0 else (far, near)
                    at = pl.multiple_of((z * RING + x) * COLS + half * (COLS // 2), COLS // 2)
                    whole[pl.ds(at, COLS // 2), :] = weights[half * RING + t][s]
        back[...] = jnp.zeros_like(back)

    @pl.when(step < RING)
    def _():
        part = whole[pl.ds(pl.multiple_of(step * TILE, TILE), TILE), :]
        back[:rows, :] += jnp.dot(cot_a[...], part, preferred_element_type=f32)
        back[rows:, :] += jnp.dot(cot_b[...], part, preferred_element_type=f32)

    @pl.when(step == RING - 1)
    def _():
        for block in range(2 * BLK):
            gate_ref, up_ref = (gate_a, up_a) if block < BLK else (gate_b, up_b)
            here = pl.ds((block % BLK) * BLOCK, BLOCK)
            gate = gate_ref[here, :].astype(f32)
            up = up_ref[here, :].astype(f32)
            sig = jax.nn.sigmoid(gate)
            value = jnp.where(row_mask(info, block, BLOCK), back[pl.ds(block * BLOCK, BLOCK), :], 0.0)
            common = value * sig
            grad_gate = common * up * (1.0 + gate * (1.0 - sig))
            grad_up = common * gate
            to = pl.ds(block * BLOCK, BLOCK)
            left[:F, to] = grad_gate.T.astype(bf16)
            left[F:, to] = grad_up.T.astype(bf16)

    @pl.when(step >= RING)
    def _():
        for m in range(2):
            one = pl.ds(m * F, F)
            acc[...] = jnp.dot(left[one, :rows], tok_a[...], preferred_element_type=f32) + jnp.dot(
                left[one, rows:], tok_b[...], preferred_element_type=f32
            )
            for half in range(2):

                @pl.when((step - RING) // 2 == half)
                def _(half=half):
                    for s in range(RING):
                        chunk = (info[half] + s) % RING
                        outs[half * RING + s][m] = acc[pl.ds(chunk * CHUNK, CHUNK), :].astype(bf16)


def sweep_kernel(info, *rest):
    parts, out, (whole, half_gram, half_poly) = rest[:8], rest[8], rest[9:]
    for half in range(2):
        for t in range(RING):
            for s in range(RING):
                near = (info[1 - half] - s) % RING
                far = (info[half] - t) % RING
                at = pl.multiple_of(far * CHUNK + near * PIECE, PIECE)
                whole[pl.ds(at, PIECE), half * HALF : (half + 1) * HALF] = parts[half * RING + t][s]
    both = (((1,), (1,)), ((), ()))
    raw = lax.dot_general(whole[...], whole[...], both, preferred_element_type=f32)
    diagonal = lax.broadcasted_iota(jnp.int32, (F, F), 0) == lax.broadcasted_iota(jnp.int32, (F, F), 1)
    norm = jnp.sqrt(jnp.sum(jnp.where(diagonal, raw, 0.0)))
    inverse = 1.0 / (norm + norm_eps)
    gram = raw * inverse * inverse

    def poly_of(gram):
        half_gram[...] = gram.astype(bf16)
        squared = jnp.dot(half_gram[...], half_gram[...], preferred_element_type=f32)
        return (ns_second * gram + ns_third * squared).astype(bf16)

    half_poly[...] = poly_of(gram)
    mixed = ns_first * gram + jnp.dot(half_poly[...], half_gram[...], preferred_element_type=f32)
    gram = ns_first * mixed + jnp.dot(mixed.astype(bf16), half_poly[...], preferred_element_type=f32)
    column = pl.multiple_of((info[0] * RING + info[1]) * COLS, COLS)
    mine = whole[:, pl.ds(column, COLS)]
    first = inverse * (
        ns_first * mine.astype(f32) + jnp.dot(half_poly[...], mine, preferred_element_type=f32)
    )
    first = first.astype(bf16)
    last = poly_of(gram)
    newer = ns_first * first.astype(f32) + jnp.dot(last, first, preferred_element_type=f32)
    out[...] = (jnp.sqrt(jnp.float32(D)) * newer).astype(bf16)


def whole_spec(shape):
    return pl.BlockSpec(shape, lambda i, info: (0,) * len(shape))


def out_spec(count, half):
    def index(i, info, first):
        return (0, 0, jnp.clip(i - first - 2 * half, 0, 1))

    return lambda first: pl.BlockSpec(
        (count, CHUNK, TILE), lambda i, info: index(i, info, first)
    )


def out_shapes(count):
    return [jax.ShapeDtypeStruct((count, CHUNK, HALF), bf16)] * 8


def chunk_specs(count, first):
    return [out_spec(count, half)(first) for half in range(2) for s in range(RING)]


def call(kernel, name, grid, in_specs, out_specs, out_shape, scratch, info, *operands):
    return pl.pallas_call(
        kernel,
        grid_spec=pltpu.PrefetchScalarGridSpec(
            num_scalar_prefetch=1,
            grid=grid,
            in_specs=in_specs,
            out_specs=out_specs,
            scratch_shapes=scratch,
        ),
        out_shape=out_shape,
        compiler_params=pltpu.CompilerParams(
            dimension_semantics=("arbitrary",), vmem_limit_bytes=56 * 1024 * 1024
        ),
        name=name,
    )(info, *operands)


AXES = ("dp_0", "dp_1")


def gather_stage(values, flip):
    found = [[values[0]], [values[1]]]
    received = {}
    for s in SHIFTS:
        for half in range(2):
            axis = AXES[1 - half] if flip else AXES[half]
            received[half, s] = shift(values[half], axis, s)
    for half in range(2):
        found[half] += [received[half, s] for s in range(1, RING)]
    return found


def per_device(token_inputs, cotangent, gate, up, down_weight, block_expert, block_count):
    z, x, c, y = (lax.axis_index(a) for a in DP_REP)
    rows = BLK * BLOCK
    turned = jnp.swapaxes(down_weight, 1, 2)
    own = lax.dynamic_index_in_dim(turned, c, 0, False)
    other = swap(lax.dynamic_index_in_dim(turned, 1 - c, 0, False))
    low = jnp.where(c == 0, own, other)
    high = jnp.where(c == 0, other, own)
    stage = gather_stage([low, high], False)
    stage = gather_stage([jnp.stack(v) for v in stage], True)
    weights = stage[0] + stage[1]

    ints = jnp.concatenate([block_count, block_expert])
    ints_b = swap(ints)
    info = jnp.concatenate(
        [
            jnp.stack([z, x, c]),
            jnp.zeros((5,), jnp.int32),
            ints[:BLK],
            ints_b[:BLK],
            ints[BLK:],
            ints_b[BLK:],
        ]
    ).astype(jnp.int32)
    gate_b, up_b, cot_b = swap(gate), swap(up), swap(cotangent)
    tok_b = swap(token_inputs)

    side = whole_spec((rows, F))
    moving = pl.BlockSpec((rows, TILE), lambda i, info: (0, i))
    hidden_out = call(
        hidden_kernel,
        "hidden_part",
        (RING,),
        [side] * 4 + [moving] * 2,
        chunk_specs(1, 0),
        out_shapes(1),
        [pltpu.VMEM((F, 2 * rows), bf16), pltpu.VMEM((F, TILE), f32)],
        info,
        gate,
        up,
        gate_b,
        up_b,
        cotangent,
        cot_b,
    )
    early = pl.BlockSpec((rows, TILE), lambda i, info: (0, jnp.minimum(i, RING - 1)))
    late = pl.BlockSpec((rows, TILE), lambda i, info: (0, jnp.maximum(i - RING, 0)))
    grads_out = call(
        grads_kernel,
        "grads_part",
        (2 * RING,),
        [side] * 4 + [early] * 2 + [late] * 2 + [whole_spec((RING, COLS // 2, F))] * 8,
        chunk_specs(2, RING),
        out_shapes(2),
        [
            pltpu.VMEM((D, F), bf16),
            pltpu.VMEM((2 * rows, F), f32),
            pltpu.VMEM((2 * F, 2 * rows), bf16),
            pltpu.VMEM((F, TILE), f32),
        ],
        info,
        gate,
        up,
        gate_b,
        up_b,
        cotangent,
        cot_b,
        token_inputs,
        tok_b,
        *weights,
    )

    def exchanged(parts, axes):
        got = {}
        for s in SHIFTS:
            for half in range(2):
                got[half, s] = shift(parts[half][s], axes[half], s)
        return [[parts[half][0]] + [got[half, s] for s in SHIFTS] for half in range(2)]

    hidden_terms = exchanged([hidden_out[:RING], hidden_out[RING:]], AXES)
    grads_terms = exchanged([grads_out[:RING], grads_out[RING:]], AXES)
    places = (x, z)

    def chunk_sum(terms, start):
        total = 0.0
        for t in terms:
            total = total + lax.dynamic_slice_in_dim(t, start, PIECE, 1).astype(f32)
        return total.astype(bf16)

    second = []
    for half in range(2):
        per_shift = []
        for s in range(RING):
            start = ((places[half] + s) % RING) * PIECE
            per_shift.append(
                jnp.concatenate(
                    [chunk_sum(grads_terms[half], start), chunk_sum(hidden_terms[half], start)], 0
                )
            )
        second.append(per_shift)
    final_terms = exchanged(second, AXES[::-1])
    halves = []
    for half in range(2):
        total = 0.0
        for t in final_terms[half]:
            total = total + t.astype(f32)
        halves.append(total.astype(bf16))
    partial_sums = jnp.stack(halves, 1)
    padded = jnp.concatenate([partial_sums, jnp.zeros((1, *partial_sums.shape[1:]), bf16)], 0)
    arrived = lax.all_to_all(padded, "rep", 0, 0, tiled=True)
    block = jnp.sum(arrived.astype(f32), axis=0).astype(bf16)

    stage = gather_stage([block[0], block[1]], True)
    stage = gather_stage([jnp.stack(v) for v in stage], False)
    update = call(
        sweep_kernel,
        "sweeps",
        (1,),
        [whole_spec((RING, PIECE, HALF))] * 8,
        whole_spec((F, COLS)),
        jax.ShapeDtypeStruct((F, COLS), bf16),
        [pltpu.VMEM((F, D), bf16), pltpu.VMEM((F, F), bf16), pltpu.VMEM((F, F), bf16)],
        info,
        *stage[0],
        *stage[1],
    )
    mine = lax.all_gather(update, "rep", axis=0)[:3]
    theirs = swap(mine)
    width = COLS // 2
    mine, theirs = (jnp.where(c == 0, v[..., :width], v[..., width:]) for v in (mine, theirs))
    return jnp.stack([jnp.where(c == 0, mine, theirs), jnp.where(c == 0, theirs, mine)], 0)


def solution(mesh):
    torus = Mesh(mesh.devices.reshape(4, 4, 2, mesh.shape["rep"]), DP_REP)
    return jax.shard_map(
        per_device,
        mesh=torus,
        in_specs=(
            P(DP_REP, None),
            P(DP_REP, None),
            P(DP_REP, None),
            P(DP_REP, None),
            P(None, None, DP),
            P(DP_REP),
            P(DP_REP),
        ),
        out_specs=P(None, None, None, DP),
        check_vma=False,
    )
```

```python
import functools

import jax
import jax.numpy as jnp
from jax import lax
from jax.experimental import pallas as pl
from jax.experimental.pallas import tpu as pltpu
from jax.sharding import Mesh
from jax.sharding import PartitionSpec as P


DP = ("dp_0", "dp_1", "dp_2")
DP_REP = ("dp_0", "dp_1", "dp_2", "rep")

ns_first = 3.4445
ns_second = -4.775
ns_third = 2.0315
norm_eps = 1e-07

F = 768
D = 2048
BLOCK = 128
BLK = 4
HALF = D // 2
TILE = 512
RING = 4
CHUNK = F // RING
PIECE = CHUNK // RING
COLS = D // 16
SHIFTS = (1, 3, 2)
f32 = jnp.float32
bf16 = jnp.bfloat16


def shift(value, axis, by, sources=RING, targets=RING):
    pairs = [(i, (i + by) % RING) for i in range(sources)]
    return lax.ppermute(value, axis, [p for p in pairs if p[1] < targets])


def swap(value):
    return lax.ppermute(value, "dp_2", [(0, 1), (1, 0)])


def turn_kernel(info, own, other, first, second, rows):
    width = COLS // 2
    here = info[2]
    rows[pl.ds(pl.multiple_of(here * width, width), width), :] = own[here].astype(f32)
    rows[pl.ds(pl.multiple_of((1 - here) * width, width), width), :] = other[here].astype(f32)
    value = rows[...].T.astype(bf16)
    first[...] = value[: F // 2]
    second[...] = value[F // 2 :]


def finish_kernel(info, *rest):
    terms, outs = rest[:8], rest[8:]
    for s in range(RING):
        matrix = (info[3] + s) % RING
        at = jnp.minimum(matrix, 2)
        for half in range(2):
            value = terms[half * RING][at].astype(f32)
            for j in range(1, RING):
                value = value + terms[half * RING + j][at].astype(f32)
            outs[s][half] = jnp.where(matrix < 3, value, 0.0).astype(bf16)


def products(half, place, left, right_a, right_b, acc, outs):
    rows = BLK * BLOCK
    mats = left.shape[0] // F

    def tile(n, carry):
        to = pl.ds(pl.multiple_of(n * TILE, TILE), TILE)
        at = pl.ds(pl.multiple_of(half * HALF + n * TILE, TILE), TILE)
        for m in range(mats):
            one = pl.ds(m * F, F)
            acc[...] = jnp.dot(
                left[one, :rows], right_a[:, at], preferred_element_type=f32
            ) + jnp.dot(left[one, rows:], right_b[:, at], preferred_element_type=f32)
            for s in range(RING):
                chunk = (place + s) % RING
                value = acc[pl.ds(pl.multiple_of(chunk * CHUNK, CHUNK), CHUNK), :]
                outs[half * RING + s][m, :, to] = value.astype(bf16)
        return carry

    lax.fori_loop(0, HALF // TILE, tile, 0)


def hidden_kernel(info, count_a, expert_a, count_b, expert_b, gate_h, up_h, cot_h, *rest):
    gate_b, up_b, cot_b = rest[:3]
    outs, for_gate, for_up = rest[3:11], rest[11], rest[12]
    gate_a, up_a, cot_a, left, acc, sems = rest[13:]
    copies = [
        pltpu.make_async_copy(source, target, sems.at[i])
        for i, (source, target) in enumerate(((gate_h, gate_a), (up_h, up_a), (cot_h, cot_a)))
    ]
    for copy in copies:
        copy.start()

    def factors(gate_ref, up_ref, count, expert, base):
        def block(i, carry):
            rows = pl.ds(pl.multiple_of(i * BLOCK, BLOCK), BLOCK)
            gate = gate_ref[rows, :].astype(f32).T
            up = up_ref[rows, :].astype(f32).T
            limit = jnp.where(expert[i] == info[2], count[i], 0)
            live = lax.broadcasted_iota(jnp.int32, (F, BLOCK), 1) < limit
            sig = jax.nn.sigmoid(gate)
            to = pl.ds(pl.multiple_of(base + i * BLOCK, BLOCK), BLOCK)
            common = jnp.where(live, sig, 0.0)
            factor = common * gate
            left[:, to] = (factor * up).astype(bf16)
            for_up[:, to] = factor.astype(bf16)
            for_gate[:, to] = (common * up * (1.0 + gate * (1.0 - sig))).astype(bf16)
            return carry

        lax.fori_loop(0, BLK, block, 0)

    factors(gate_b, up_b, count_b, expert_b, BLK * BLOCK)
    copies[0].wait()
    copies[1].wait()
    factors(gate_a, up_a, count_a, expert_a, 0)
    copies[2].wait()
    for half in range(2):
        products(half, info[half], left, cot_a, cot_b, acc, outs)


def grads_kernel(info, cot_h, tok_h, for_gate, for_up, cot_b, tok_b, *rest):
    weights, outs, (cot_a, tok_a, whole, left, acc, sems) = rest[:8], rest[8:16], rest[16:]
    rows = BLK * BLOCK
    part = rows // 2
    halves = F // 2
    copies = [
        pltpu.make_async_copy(source, target, sems.at[i])
        for i, (source, target) in enumerate(((cot_h, cot_a), (tok_h, tok_a)))
    ]
    for copy in copies:
        copy.start()
    for half in range(2):
        for t in range(RING):
            for s in range(RING):
                near = (info[half] - s) % RING
                far = (info[1 - half] - t) % RING
                z, x = (near, far) if half == 0 else (far, near)
                at = pl.multiple_of((z * RING + x) * COLS, COLS)
                whole[half * halves : (half + 1) * halves, pl.ds(at, COLS)] = weights[
                    half * RING + t
                ][s]

    def backward(cot, base):
        def step(i, carry):
            here = pl.ds(pl.multiple_of(i * part, part), part)
            to = pl.ds(pl.multiple_of(base + i * part, part), part)
            back = lax.dot_general(
                whole[...], cot[here, :], (((1,), (1,)), ((), ())), preferred_element_type=f32
            )
            left[:F, to] = (back * for_gate[:, to].astype(f32)).astype(bf16)
            left[F:, to] = (back * for_up[:, to].astype(f32)).astype(bf16)
            return carry

        lax.fori_loop(0, rows // part, step, 0)

    backward(cot_b, rows)
    copies[0].wait()
    backward(cot_a, 0)
    copies[1].wait()
    for half in range(2):
        products(half, info[half], left, tok_a, tok_b, acc, outs)


def fold_kernel(half, info, *rest):
    grads, hidden, outs = rest[:4], rest[4:8], rest[8:]
    place = info[1 - half]

    def total(terms, at):
        value = terms[0][:, at, :].astype(f32)
        for term in terms[1:]:
            value = value + term[:, at, :].astype(f32)
        return value.astype(bf16)

    for s in range(RING):
        at = pl.ds(pl.multiple_of(((place + s) % RING) * PIECE, PIECE), PIECE)
        outs[s][:2] = total(grads, at)
        outs[s][2:] = total(hidden, at)


def settle_kernel(info, *rest):
    terms, outs = rest[:RING], rest[RING:]
    for half in range(2):
        value = terms[0][half].astype(f32)
        for term in terms[1:]:
            value = value + term[half].astype(f32)
        outs[half][...] = value.astype(bf16)


def pair_kernel(info, kept, arrived, out):
    out[info[2]] = kept[...]
    out[1 - info[2]] = arrived[...]


def spread_kernel(info, *rest):
    pieces, out = rest[:RING], rest[RING]
    for s in range(RING):
        matrix = (info[3] - s) % RING

        @pl.when(matrix < 3)
        def _(s=s, matrix=matrix):
            for expert in range(2):
                out[expert, matrix] = pieces[s][expert]


def sweep_kernel(info, *rest):
    parts, kept, sent, (whole, half_gram, half_poly, turned) = rest[:8], rest[8], rest[9], rest[10:]
    for half in range(2):
        for t in range(RING):
            for s in range(RING):
                near = (info[1 - half] - s) % RING
                far = (info[half] - t) % RING
                at = pl.multiple_of(far * CHUNK + near * PIECE, PIECE)
                whole[pl.ds(at, PIECE), half * HALF : (half + 1) * HALF] = parts[half * RING + t][s]
    both = (((1,), (1,)), ((), ()))
    raw = lax.dot_general(whole[...], whole[...], both, preferred_element_type=f32)
    diagonal = lax.broadcasted_iota(jnp.int32, (F, F), 0) == lax.broadcasted_iota(jnp.int32, (F, F), 1)
    norm = jnp.sqrt(jnp.sum(jnp.where(diagonal, raw, 0.0)))
    inverse = 1.0 / (norm + norm_eps)
    gram = raw * inverse * inverse

    def poly_of(gram):
        half_gram[...] = gram.astype(bf16)
        squared = jnp.dot(half_gram[...], half_gram[...], preferred_element_type=f32)
        return (ns_second * gram + ns_third * squared).astype(bf16)

    half_poly[...] = poly_of(gram)
    mixed = ns_first * gram + jnp.dot(half_poly[...], half_gram[...], preferred_element_type=f32)
    gram = ns_first * mixed + jnp.dot(mixed.astype(bf16), half_poly[...], preferred_element_type=f32)
    column = pl.multiple_of((info[0] * RING + info[1]) * COLS, COLS)
    mine = whole[:, pl.ds(column, COLS)]
    first = inverse * (
        ns_first * mine.astype(f32) + jnp.dot(half_poly[...], mine, preferred_element_type=f32)
    )
    first = first.astype(bf16)
    last = poly_of(gram)
    newer = ns_first * first.astype(f32) + jnp.dot(last, first, preferred_element_type=f32)
    turned[...] = (jnp.sqrt(jnp.float32(D)) * newer).T
    width = COLS // 2
    for ref, core in ((kept, info[2]), (sent, 1 - info[2])):
        ref[...] = turned[pl.ds(pl.multiple_of(core * width, width), width), :].astype(bf16)


def out_shapes(count):
    return [jax.ShapeDtypeStruct((count, CHUNK, HALF), bf16)] * 8


def call(kernel, flops, room, out_shape, scratch, scalars, operands, far=0):
    several = isinstance(out_shape, list)
    operands = [
        pltpu.with_memory_space_constraint(v, pltpu.HBM) if i < far else v
        for i, v in enumerate(operands)
    ]
    specs = [pl.BlockSpec(memory_space=pltpu.HBM)] * far
    specs += [pl.BlockSpec(memory_space=pltpu.VMEM)] * (len(operands) - far)
    out_spec = pl.BlockSpec(memory_space=pltpu.VMEM)
    return pl.pallas_call(
        kernel,
        in_specs=[pl.BlockSpec(memory_space=pltpu.SMEM)] * len(scalars) + specs,
        out_specs=[out_spec] * len(out_shape) if several else out_spec,
        out_shape=out_shape,
        scratch_shapes=scratch,
        compiler_params=pltpu.CompilerParams(vmem_limit_bytes=room * 1024 * 1024),
        cost_estimate=pl.CostEstimate(flops=flops, bytes_accessed=flops // 500, transcendentals=0),
    )(*scalars, *operands)


AXES = ("dp_0", "dp_1")


def gather_stage(values, flip):
    found = [[values[0]], [values[1]]]
    received = {}
    for s in SHIFTS:
        for half in range(2):
            axis = AXES[1 - half] if flip else AXES[half]
            received[half, s] = shift(values[half], axis, s)
    for half in range(2):
        found[half] += [received[half, s] for s in range(1, RING)]
    return found


def per_device(token_inputs, cotangent, gate, up, down_weight, block_expert, block_count):
    z, x, c, y = (lax.axis_index(a) for a in DP_REP)
    rows = BLK * BLOCK
    turned = jnp.swapaxes(down_weight, 1, 2)
    other = swap(turned)
    info = jnp.stack([z, x, c, y]).astype(jnp.int32)
    columns = call(
        turn_kernel,
        F * D,
        4,
        [jax.ShapeDtypeStruct((F // 2, COLS), bf16)] * 2,
        [pltpu.VMEM((COLS, F), f32)],
        [info],
        [turned, other],
    )
    count_b, expert_b = swap(block_count), swap(block_expert)
    columns, gate, up, cotangent, token_inputs, count_b, expert_b = lax.optimization_barrier(
        (columns, gate, up, cotangent, token_inputs, count_b, expert_b)
    )
    stage = gather_stage(columns, False)
    stacked = [jnp.stack(v) for v in stage]
    stage = gather_stage(stacked, True)
    weights = stage[0] + stage[1]

    gate_b, up_b = swap(gate), swap(up)
    cot_b, tok_b = swap(cotangent), swap(token_inputs)

    factor_shape = jax.ShapeDtypeStruct((F, 2 * rows), bf16)
    *hidden_out, for_gate, for_up = call(
        hidden_kernel,
        2 * F * 2 * rows * D,
        12,
        out_shapes(1) + [factor_shape] * 2,
        [
            pltpu.VMEM((rows, F), bf16),
            pltpu.VMEM((rows, F), bf16),
            pltpu.VMEM((rows, D), bf16),
            pltpu.VMEM((F, 2 * rows), bf16),
            pltpu.VMEM((F, TILE), f32),
            pltpu.SemaphoreType.DMA((3,)),
        ],
        [info, block_count, block_expert, count_b, expert_b],
        [gate, up, cotangent, gate_b, up_b, cot_b],
        3,
    )
    grads_out = call(
        grads_kernel,
        6 * F * 2 * rows * D,
        18,
        out_shapes(2),
        [
            pltpu.VMEM((rows, D), bf16),
            pltpu.VMEM((rows, D), bf16),
            pltpu.VMEM((F, D), bf16),
            pltpu.VMEM((2 * F, 2 * rows), bf16),
            pltpu.VMEM((F, TILE), f32),
            pltpu.SemaphoreType.DMA((2,)),
        ],
        [info],
        [cotangent, token_inputs, for_gate, for_up, cot_b, tok_b, *weights],
        2,
    )

    def exchanged(parts, axes):
        got = {}
        for s in SHIFTS:
            for half in range(2):
                got[half, s] = shift(parts[half][s], axes[half], s)
        return [[parts[half][0]] + [got[half, s] for s in SHIFTS] for half in range(2)]

    hidden_terms = exchanged([hidden_out[:RING], hidden_out[RING:]], AXES)
    grads_terms = exchanged([grads_out[:RING], grads_out[RING:]], AXES)

    def fold(half):
        return call(
            functools.partial(fold_kernel, half),
            F * HALF * RING,
            4,
            [jax.ShapeDtypeStruct((3, PIECE, HALF), bf16)] * 4,
            [],
            [info],
            [*grads_terms[half], *hidden_terms[half]],
        )

    second = [fold(half) for half in range(2)]
    final_terms = exchanged(second, AXES[::-1])
    blocks = (2, PIECE, HALF)
    parts = call(
        finish_kernel,
        F * D,
        4,
        [jax.ShapeDtypeStruct(blocks, bf16)] * RING,
        [],
        [info],
        [*final_terms[0], *final_terms[1]],
    )
    arrived = [shift(parts[s], "rep", s, targets=3) for s in SHIFTS]
    block = call(
        settle_kernel,
        F * D,
        4,
        [jax.ShapeDtypeStruct((PIECE, HALF), bf16)] * 2,
        [],
        [info],
        [parts[0], *arrived],
    )
    stage = gather_stage([block[0], block[1]], True)
    stage = gather_stage([jnp.stack(v) for v in stage], False)
    kept, sent = call(
        sweep_kernel,
        8 * F * F * F,
        26,
        [jax.ShapeDtypeStruct((COLS // 2, F), bf16)] * 2,
        [
            pltpu.VMEM((F, D), bf16),
            pltpu.VMEM((F, F), bf16),
            pltpu.VMEM((F, F), bf16),
            pltpu.VMEM((COLS, F), f32),
        ],
        [info],
        [*stage[0], *stage[1]],
    )
    narrow = (2, COLS // 2, F)
    pair = call(
        pair_kernel, F * COLS, 2, jax.ShapeDtypeStruct(narrow, bf16), [], [info], [kept, swap(sent)]
    )
    pieces = {0: pair, **{s: shift(pair, "rep", s, sources=3) for s in SHIFTS}}
    everyone = call(
        spread_kernel,
        F * COLS,
        4,
        jax.ShapeDtypeStruct((2, 3, COLS // 2, F), bf16),
        [],
        [info],
        [pieces[s] for s in range(RING)],
    )
    return jnp.swapaxes(everyone, 2, 3)


def solution(mesh):
    torus = Mesh(mesh.devices.reshape(4, 4, 2, mesh.shape["rep"]), DP_REP)

    return jax.shard_map(
        per_device,
        mesh=torus,
        in_specs=(
            P(DP_REP, None),
            P(DP_REP, None),
            P(DP_REP, None),
            P(DP_REP, None),
            P(None, None, DP),
            P(DP_REP),
            P(DP_REP),
        ),
        out_specs=P(None, None, None, DP),
        check_vma=False,
    )
```

```python
import functools

import jax
import jax.numpy as jnp
from jax import lax
from jax.experimental import pallas as pl
from jax.experimental.pallas import tpu as pltpu
from jax.sharding import Mesh
from jax.sharding import PartitionSpec as P


DP = ("dp_0", "dp_1", "dp_2")
DP_REP = ("dp_0", "dp_1", "dp_2", "rep")

ns_first = 3.4445
ns_second = -4.775
ns_third = 2.0315
norm_eps = 1e-07

F = 768
D = 2048
BLOCK = 128
BLK = 4
HALF = D // 2
TILE = 512
RING = 4
CHUNK = F // RING
PIECE = CHUNK // RING
COLS = D // 16
SHIFTS = (1, 3, 2)
f32 = jnp.float32
bf16 = jnp.bfloat16


def shift(value, axis, by):
    return lax.ppermute(value, axis, [(i, (i + by) % RING) for i in range(RING)])


def swap(value):
    return lax.ppermute(value, "dp_2", [(0, 1), (1, 0)])


def turn_kernel(info, own, other, first, second, rows):
    width = COLS // 2
    here = info[2]
    rows[pl.ds(pl.multiple_of(here * width, width), width), :] = own[...].astype(f32)
    rows[pl.ds(pl.multiple_of((1 - here) * width, width), width), :] = other[here].astype(f32)
    value = rows[...].T.astype(bf16)
    first[...] = value[: F // 2]
    second[...] = value[F // 2 :]


def finish_kernel(info, *rest):
    terms, outs = rest[:8], rest[8:]
    for s in range(RING):
        matrix = (info[3] + s) % RING
        at = jnp.minimum(matrix, 2)
        for half in range(2):
            value = terms[half * RING][at].astype(f32)
            for j in range(1, RING):
                value = value + terms[half * RING + j][at].astype(f32)
            outs[s][half] = jnp.where(matrix < 3, value, 0.0).astype(bf16)


def products(half, place, left, right_a, right_b, acc, outs):
    rows = BLK * BLOCK
    mats = left.shape[0] // F

    def tile(n, carry):
        to = pl.ds(pl.multiple_of(n * TILE, TILE), TILE)
        at = pl.ds(pl.multiple_of(half * HALF + n * TILE, TILE), TILE)
        for m in range(mats):
            one = pl.ds(m * F, F)
            acc[...] = jnp.dot(
                left[one, :rows], right_a[:, at], preferred_element_type=f32
            ) + jnp.dot(left[one, rows:], right_b[:, at], preferred_element_type=f32)
            for s in range(RING):
                chunk = (place + s) % RING
                value = acc[pl.ds(pl.multiple_of(chunk * CHUNK, CHUNK), CHUNK), :]
                outs[half * RING + s][m, :, to] = value.astype(bf16)
        return carry

    lax.fori_loop(0, HALF // TILE, tile, 0)


def hidden_kernel(info, count_a, expert_a, count_b, expert_b, gate_h, up_h, cot_h, *rest):
    gate_b, up_b, cot_b = rest[:3]
    outs, for_gate, for_up = rest[3:11], rest[11], rest[12]
    gate_a, up_a, cot_a, left, acc, sems = rest[13:]
    copies = [
        pltpu.make_async_copy(source, target, sems.at[i])
        for i, (source, target) in enumerate(((gate_h, gate_a), (up_h, up_a), (cot_h, cot_a)))
    ]
    for copy in copies:
        copy.start()

    def factors(gate_ref, up_ref, count, expert, base):
        def block(i, carry):
            rows = pl.ds(pl.multiple_of(i * BLOCK, BLOCK), BLOCK)
            gate = gate_ref[rows, :].astype(f32).T
            up = up_ref[rows, :].astype(f32).T
            limit = jnp.where(expert[i] == info[2], count[i], 0)
            live = lax.broadcasted_iota(jnp.int32, (F, BLOCK), 1) < limit
            sig = jax.nn.sigmoid(gate)
            to = pl.ds(pl.multiple_of(base + i * BLOCK, BLOCK), BLOCK)
            common = jnp.where(live, sig, 0.0)
            factor = common * gate
            left[:, to] = (factor * up).astype(bf16)
            for_up[:, to] = factor.astype(bf16)
            for_gate[:, to] = (common * up * (1.0 + gate * (1.0 - sig))).astype(bf16)
            return carry

        lax.fori_loop(0, BLK, block, 0)

    factors(gate_b, up_b, count_b, expert_b, BLK * BLOCK)
    copies[0].wait()
    copies[1].wait()
    factors(gate_a, up_a, count_a, expert_a, 0)
    copies[2].wait()
    for half in range(2):
        products(half, info[half], left, cot_a, cot_b, acc, outs)


def grads_kernel(info, cot_h, tok_h, for_gate, for_up, cot_b, tok_b, *rest):
    weights, outs, (cot_a, tok_a, whole, left, acc, sems) = rest[:8], rest[8:16], rest[16:]
    rows = BLK * BLOCK
    part = rows // 2
    halves = F // 2
    copies = [
        pltpu.make_async_copy(source, target, sems.at[i])
        for i, (source, target) in enumerate(((cot_h, cot_a), (tok_h, tok_a)))
    ]
    for copy in copies:
        copy.start()
    for half in range(2):
        for t in range(RING):
            for s in range(RING):
                near = (info[half] - s) % RING
                far = (info[1 - half] - t) % RING
                z, x = (near, far) if half == 0 else (far, near)
                at = pl.multiple_of((z * RING + x) * COLS, COLS)
                whole[half * halves : (half + 1) * halves, pl.ds(at, COLS)] = weights[
                    half * RING + t
                ][s]

    def backward(cot, base):
        def step(i, carry):
            here = pl.ds(pl.multiple_of(i * part, part), part)
            to = pl.ds(pl.multiple_of(base + i * part, part), part)
            back = lax.dot_general(
                whole[...], cot[here, :], (((1,), (1,)), ((), ())), preferred_element_type=f32
            )
            left[:F, to] = (back * for_gate[:, to].astype(f32)).astype(bf16)
            left[F:, to] = (back * for_up[:, to].astype(f32)).astype(bf16)
            return carry

        lax.fori_loop(0, rows // part, step, 0)

    backward(cot_b, rows)
    copies[0].wait()
    backward(cot_a, 0)
    copies[1].wait()
    for half in range(2):
        products(half, info[half], left, tok_a, tok_b, acc, outs)


def fold_kernel(half, info, *rest):
    grads, hidden, outs = rest[:4], rest[4:8], rest[8:]
    place = info[1 - half]

    def total(terms, at):
        value = terms[0][:, at, :].astype(f32)
        for term in terms[1:]:
            value = value + term[:, at, :].astype(f32)
        return value.astype(bf16)

    for s in range(RING):
        at = pl.ds(pl.multiple_of(((place + s) % RING) * PIECE, PIECE), PIECE)
        outs[s][:2] = total(grads, at)
        outs[s][2:] = total(hidden, at)


def settle_kernel(info, *rest):
    terms, outs = rest[:RING], rest[RING:]
    for half in range(2):
        value = terms[0][half].astype(f32)
        for term in terms[1:]:
            value = value + term[half].astype(f32)
        outs[half][...] = value.astype(bf16)


def pair_kernel(info, kept, arrived, out):
    out[info[2]] = kept[...]
    out[1 - info[2]] = arrived[...]


def spread_kernel(info, *rest):
    pieces, out = rest[:RING], rest[RING]
    for s in range(RING):
        matrix = (info[3] - s) % RING

        @pl.when(matrix < 3)
        def _(s=s, matrix=matrix):
            for expert in range(2):
                out[expert, matrix] = pieces[s][expert]


def put_half(half, info, parts, whole):
    for t in range(RING):
        for s in range(RING):
            near = (info[1 - half] - s) % RING
            far = (info[half] - t) % RING
            at = pl.multiple_of(far * CHUNK + near * PIECE, PIECE)
            whole[pl.ds(at, PIECE), :] = parts[t][s]


def self_product(ref):
    return lax.dot_general(ref[...], ref[...], (((1,), (1,)), ((), ())), preferred_element_type=f32)


def gram_kernel(info, *rest):
    parts, (raw, first_half) = rest[:RING], rest[RING:]
    put_half(0, info, parts, first_half)
    raw[...] = self_product(first_half)


def sweep_kernel(info, raw_first, first_half, *rest):
    parts, kept, sent = rest[:RING], rest[RING], rest[RING + 1]
    second_half, half_gram, half_poly, turned, block = rest[RING + 2 :]
    put_half(1, info, parts, second_half)
    raw = raw_first[...] + self_product(second_half)
    diagonal = lax.broadcasted_iota(jnp.int32, (F, F), 0) == lax.broadcasted_iota(jnp.int32, (F, F), 1)
    norm = jnp.sqrt(jnp.sum(jnp.where(diagonal, raw, 0.0)))
    inverse = 1.0 / (norm + norm_eps)
    gram = raw * inverse * inverse

    def poly_of(gram):
        half_gram[...] = gram.astype(bf16)
        squared = jnp.dot(half_gram[...], half_gram[...], preferred_element_type=f32)
        return (ns_second * gram + ns_third * squared).astype(bf16)

    half_poly[...] = poly_of(gram)
    mixed = ns_first * gram + jnp.dot(half_poly[...], half_gram[...], preferred_element_type=f32)
    gram = ns_first * mixed + jnp.dot(mixed.astype(bf16), half_poly[...], preferred_element_type=f32)
    place = info[0] * RING + info[1]
    column = pl.multiple_of((place % (HALF // COLS)) * COLS, COLS)
    for half, ref in ((0, first_half), (1, second_half)):

        @pl.when(place // (HALF // COLS) == half)
        def _(ref=ref):
            block[...] = ref[:, pl.ds(column, COLS)]

    mine = block[...]
    first = inverse * (
        ns_first * mine.astype(f32) + jnp.dot(half_poly[...], mine, preferred_element_type=f32)
    )
    first = first.astype(bf16)
    last = poly_of(gram)
    newer = ns_first * first.astype(f32) + jnp.dot(last, first, preferred_element_type=f32)
    turned[...] = (jnp.sqrt(jnp.float32(D)) * newer).T
    width = COLS // 2
    for ref, core in ((kept, info[2]), (sent, 1 - info[2])):
        ref[...] = turned[pl.ds(pl.multiple_of(core * width, width), width), :].astype(bf16)


def out_shapes(count):
    return [jax.ShapeDtypeStruct((count, CHUNK, HALF), bf16)] * 8


def call(kernel, flops, room, out_shape, scratch, scalars, operands, far=0):
    several = isinstance(out_shape, list)
    operands = [
        pltpu.with_memory_space_constraint(v, pltpu.HBM) if i < far else v
        for i, v in enumerate(operands)
    ]
    specs = [pl.BlockSpec(memory_space=pltpu.HBM)] * far
    specs += [pl.BlockSpec(memory_space=pltpu.VMEM)] * (len(operands) - far)
    out_spec = pl.BlockSpec(memory_space=pltpu.VMEM)
    return pl.pallas_call(
        kernel,
        in_specs=[pl.BlockSpec(memory_space=pltpu.SMEM)] * len(scalars) + specs,
        out_specs=[out_spec] * len(out_shape) if several else out_spec,
        out_shape=out_shape,
        scratch_shapes=scratch,
        compiler_params=pltpu.CompilerParams(vmem_limit_bytes=room * 1024 * 1024),
        cost_estimate=pl.CostEstimate(flops=flops, bytes_accessed=flops // 500, transcendentals=0),
    )(*scalars, *operands)


AXES = ("dp_0", "dp_1")


def gather_stage(values, flip):
    found = [[values[0]], [values[1]]]
    received = {}
    for s in SHIFTS:
        for half in range(2):
            axis = AXES[1 - half] if flip else AXES[half]
            received[half, s] = shift(values[half], axis, s)
    for half in range(2):
        found[half] += [received[half, s] for s in range(1, RING)]
    return found


def per_device(token_inputs, cotangent, gate, up, down_weight, block_expert, block_count):
    z, x, c, y = (lax.axis_index(a) for a in DP_REP)
    rows = BLK * BLOCK
    turned = jnp.swapaxes(down_weight, 1, 2)
    other = swap(turned)
    own = lax.dynamic_index_in_dim(turned, c, 0, False)
    info = jnp.stack([z, x, c, y]).astype(jnp.int32)
    columns = call(
        turn_kernel,
        F * D,
        4,
        [jax.ShapeDtypeStruct((F // 2, COLS), bf16)] * 2,
        [pltpu.VMEM((COLS, F), f32)],
        [info],
        [own, other],
    )
    count_b, expert_b = swap(block_count), swap(block_expert)
    columns, gate, up, cotangent, token_inputs, count_b, expert_b = lax.optimization_barrier(
        (columns, gate, up, cotangent, token_inputs, count_b, expert_b)
    )
    stage = gather_stage(columns, False)
    stacked = [jnp.stack(v) for v in stage]
    stage = gather_stage(stacked, True)
    weights = stage[0] + stage[1]

    gate_b, up_b = swap(gate), swap(up)
    cot_b, tok_b = swap(cotangent), swap(token_inputs)

    factor_shape = jax.ShapeDtypeStruct((F, 2 * rows), bf16)
    *hidden_out, for_gate, for_up = call(
        hidden_kernel,
        2 * F * 2 * rows * D,
        12,
        out_shapes(1) + [factor_shape] * 2,
        [
            pltpu.VMEM((rows, F), bf16),
            pltpu.VMEM((rows, F), bf16),
            pltpu.VMEM((rows, D), bf16),
            pltpu.VMEM((F, 2 * rows), bf16),
            pltpu.VMEM((F, TILE), f32),
            pltpu.SemaphoreType.DMA((3,)),
        ],
        [info, block_count, block_expert, count_b, expert_b],
        [gate, up, cotangent, gate_b, up_b, cot_b],
        3,
    )
    grads_out = call(
        grads_kernel,
        6 * F * 2 * rows * D,
        18,
        out_shapes(2),
        [
            pltpu.VMEM((rows, D), bf16),
            pltpu.VMEM((rows, D), bf16),
            pltpu.VMEM((F, D), bf16),
            pltpu.VMEM((2 * F, 2 * rows), bf16),
            pltpu.VMEM((F, TILE), f32),
            pltpu.SemaphoreType.DMA((2,)),
        ],
        [info],
        [cotangent, token_inputs, for_gate, for_up, cot_b, tok_b, *weights],
        2,
    )

    def exchanged(parts, axes):
        got = {}
        for s in SHIFTS:
            for half in range(2):
                got[half, s] = shift(parts[half][s], axes[half], s)
        return [[parts[half][0]] + [got[half, s] for s in SHIFTS] for half in range(2)]

    hidden_terms = exchanged([hidden_out[:RING], hidden_out[RING:]], AXES)
    grads_terms = exchanged([grads_out[:RING], grads_out[RING:]], AXES)

    def fold(half):
        return call(
            functools.partial(fold_kernel, half),
            F * HALF * RING,
            4,
            [jax.ShapeDtypeStruct((3, PIECE, HALF), bf16)] * 4,
            [],
            [info],
            [*grads_terms[half], *hidden_terms[half]],
        )

    second = [fold(half) for half in range(2)]
    final_terms = exchanged(second, AXES[::-1])
    blocks = (2, PIECE, HALF)
    parts = call(
        finish_kernel,
        F * D,
        4,
        [jax.ShapeDtypeStruct(blocks, bf16)] * RING,
        [],
        [info],
        [*final_terms[0], *final_terms[1]],
    )
    arrived = [shift(parts[s], "rep", s) for s in SHIFTS]
    block = call(
        settle_kernel,
        F * D,
        4,
        [jax.ShapeDtypeStruct((PIECE, HALF), bf16)] * 2,
        [],
        [info],
        [parts[0], *arrived],
    )
    stage = gather_stage(block, True)
    stage = gather_stage([jnp.stack(v) for v in stage], False)
    raw, first_half = call(
        gram_kernel,
        F * F * D,
        8,
        [jax.ShapeDtypeStruct((F, F), f32), jax.ShapeDtypeStruct((F, HALF), bf16)],
        [],
        [info],
        stage[0],
    )
    kept, sent = call(
        sweep_kernel,
        8 * F * F * F,
        26,
        [jax.ShapeDtypeStruct((COLS // 2, F), bf16)] * 2,
        [
            pltpu.VMEM((F, HALF), bf16),
            pltpu.VMEM((F, F), bf16),
            pltpu.VMEM((F, F), bf16),
            pltpu.VMEM((COLS, F), f32),
            pltpu.VMEM((F, COLS), bf16),
        ],
        [info],
        [raw, first_half, *stage[1]],
    )
    narrow = (2, COLS // 2, F)
    pair = call(
        pair_kernel, F * COLS, 2, jax.ShapeDtypeStruct(narrow, bf16), [], [info], [kept, swap(sent)]
    )
    pieces = {0: pair, **{s: shift(pair, "rep", s) for s in SHIFTS}}
    everyone = call(
        spread_kernel,
        F * COLS,
        4,
        jax.ShapeDtypeStruct((2, 3, COLS // 2, F), bf16),
        [],
        [info],
        [pieces[s] for s in range(RING)],
    )
    return jnp.swapaxes(everyone, 2, 3)


def solution(mesh):
    torus = Mesh(mesh.devices.reshape(4, 4, 2, mesh.shape["rep"]), DP_REP)

    return jax.shard_map(
        per_device,
        mesh=torus,
        in_specs=(
            P(DP_REP, None),
            P(DP_REP, None),
            P(DP_REP, None),
            P(DP_REP, None),
            P(None, None, DP),
            P(DP_REP),
            P(DP_REP),
        ),
        out_specs=P(None, None, None, DP),
        check_vma=False,
    )
```

```python
import functools

import jax
import jax.numpy as jnp
from jax import lax
from jax.experimental import pallas as pl
from jax.experimental.pallas import tpu as pltpu
from jax.sharding import Mesh
from jax.sharding import PartitionSpec as P


DP = ("dp_0", "dp_1", "dp_2")
DP_REP = ("dp_0", "dp_1", "dp_2", "rep")

ns_first = 3.4445
ns_second = -4.775
ns_third = 2.0315
norm_eps = 1e-07

F = 768
D = 2048
BLOCK = 128
BLK = 4
HALF = D // 2
TILE = 512
RING = 4
CHUNK = F // RING
PIECE = CHUNK // RING
COLS = D // 16
SHIFTS = (1, 3, 2)
f32 = jnp.float32
bf16 = jnp.bfloat16


def shift(value, axis, by):
    return lax.ppermute(value, axis, [(i, (i + by) % RING) for i in range(RING)])


def swap(value):
    return lax.ppermute(value, "dp_2", [(0, 1), (1, 0)])


def turn_kernel(info, own, other, first, second, rows):
    width = COLS // 2
    here = info[2]
    rows[pl.ds(pl.multiple_of(here * width, width), width), :] = own[...].astype(f32)
    rows[pl.ds(pl.multiple_of((1 - here) * width, width), width), :] = other[here].astype(f32)
    value = rows[...].T.astype(bf16)
    first[...] = value[: F // 2]
    second[...] = value[F // 2 :]


def finish_kernel(info, *rest):
    terms, outs = rest[:8], rest[8:]
    for s in range(RING):
        matrix = (info[3] + s) % RING
        at = jnp.minimum(matrix, 2)
        for half in range(2):
            value = terms[half * RING][at].astype(f32)
            for j in range(1, RING):
                value = value + terms[half * RING + j][at].astype(f32)
            outs[s][half] = jnp.where(matrix < 3, value, 0.0).astype(bf16)


def products(half, place, left, right_a, right_b, acc, outs):
    rows = BLK * BLOCK
    mats = left.shape[0] // F

    def tile(n, carry):
        to = pl.ds(pl.multiple_of(n * TILE, TILE), TILE)
        at = pl.ds(pl.multiple_of(half * HALF + n * TILE, TILE), TILE)
        for m in range(mats):
            one = pl.ds(m * F, F)
            acc[...] = jnp.dot(
                left[one, :rows], right_a[:, at], preferred_element_type=f32
            ) + jnp.dot(left[one, rows:], right_b[:, at], preferred_element_type=f32)
            for s in range(RING):
                chunk = (place + s) % RING
                value = acc[pl.ds(pl.multiple_of(chunk * CHUNK, CHUNK), CHUNK), :]
                outs[half * RING + s][m, :, to] = value.astype(bf16)
        return carry

    lax.fori_loop(0, HALF // TILE, tile, 0)


def hidden_kernel(info, count_a, expert_a, count_b, expert_b, gate_h, up_h, cot_h, *rest):
    gate_b, up_b, cot_b = rest[:3]
    outs, for_gate, for_up = rest[3:11], rest[11], rest[12]
    gate_a, up_a, cot_a, left, acc, sems = rest[13:]
    copies = [
        pltpu.make_async_copy(source, target, sems.at[i])
        for i, (source, target) in enumerate(((gate_h, gate_a), (up_h, up_a), (cot_h, cot_a)))
    ]
    for copy in copies:
        copy.start()

    def factors(gate_ref, up_ref, count, expert, base):
        def block(i, carry):
            rows = pl.ds(pl.multiple_of(i * BLOCK, BLOCK), BLOCK)
            gate = gate_ref[rows, :].astype(f32).T
            up = up_ref[rows, :].astype(f32).T
            limit = jnp.where(expert[i] == info[2], count[i], 0)
            live = lax.broadcasted_iota(jnp.int32, (F, BLOCK), 1) < limit
            sig = jax.nn.sigmoid(gate)
            to = pl.ds(pl.multiple_of(base + i * BLOCK, BLOCK), BLOCK)
            common = jnp.where(live, sig, 0.0)
            factor = common * gate
            left[:, to] = (factor * up).astype(bf16)
            for_up[:, to] = factor.astype(bf16)
            for_gate[:, to] = (common * up * (1.0 + gate * (1.0 - sig))).astype(bf16)
            return carry

        lax.fori_loop(0, BLK, block, 0)

    factors(gate_b, up_b, count_b, expert_b, BLK * BLOCK)
    copies[0].wait()
    copies[1].wait()
    factors(gate_a, up_a, count_a, expert_a, 0)
    copies[2].wait()
    for half in range(2):
        products(half, info[half], left, cot_a, cot_b, acc, outs)


def grads_kernel(info, cot_h, tok_h, for_gate, for_up, cot_b, tok_b, *rest):
    weights, outs, (cot_a, tok_a, whole, left, acc, sems) = rest[:8], rest[8:16], rest[16:]
    rows = BLK * BLOCK
    part = rows // 2
    halves = F // 2
    copies = [
        pltpu.make_async_copy(source, target, sems.at[i])
        for i, (source, target) in enumerate(((cot_h, cot_a), (tok_h, tok_a)))
    ]
    for copy in copies:
        copy.start()
    for half in range(2):
        for t in range(RING):
            for s in range(RING):
                near = (info[half] - s) % RING
                far = (info[1 - half] - t) % RING
                z, x = (near, far) if half == 0 else (far, near)
                at = pl.multiple_of((z * RING + x) * COLS, COLS)
                whole[half * halves : (half + 1) * halves, pl.ds(at, COLS)] = weights[
                    half * RING + t
                ][s]

    def backward(cot, base):
        def step(i, carry):
            here = pl.ds(pl.multiple_of(i * part, part), part)
            to = pl.ds(pl.multiple_of(base + i * part, part), part)
            back = lax.dot_general(
                whole[...], cot[here, :], (((1,), (1,)), ((), ())), preferred_element_type=f32
            )
            left[:F, to] = (back * for_gate[:, to].astype(f32)).astype(bf16)
            left[F:, to] = (back * for_up[:, to].astype(f32)).astype(bf16)
            return carry

        lax.fori_loop(0, rows // part, step, 0)

    backward(cot_b, rows)
    copies[0].wait()
    backward(cot_a, 0)
    copies[1].wait()
    for half in range(2):
        products(half, info[half], left, tok_a, tok_b, acc, outs)


def fold_kernel(half, info, *rest):
    grads, hidden, outs = rest[:4], rest[4:8], rest[8:]
    place = info[1 - half]

    def total(terms, at):
        value = terms[0][:, at, :].astype(f32)
        for term in terms[1:]:
            value = value + term[:, at, :].astype(f32)
        return value.astype(bf16)

    for s in range(RING):
        at = pl.ds(pl.multiple_of(((place + s) % RING) * PIECE, PIECE), PIECE)
        outs[s][:2] = total(grads, at)
        outs[s][2:] = total(hidden, at)


def settle_kernel(info, *rest):
    terms, outs = rest[:RING], rest[RING:]
    for half in range(2):
        value = terms[0][half].astype(f32)
        for term in terms[1:]:
            value = value + term[half].astype(f32)
        outs[half][...] = value.astype(bf16)


def pair_kernel(info, kept, arrived, out):
    out[info[2]] = kept[...]
    out[1 - info[2]] = arrived[...]


def spread_kernel(info, *rest):
    pieces, out, sems = rest[:RING], rest[RING], rest[RING + 1]

    def copies(s):
        matrix = jnp.minimum((info[3] - s) % RING, 2)
        return [
            pltpu.make_async_copy(pieces[s].at[e], out.at[e, matrix], sems.at[s, e])
            for e in range(2)
        ]

    for finish in (False, True):
        for s in range(RING):

            @pl.when((info[3] - s) % RING < 3)
            def _(s=s, finish=finish):
                for copy in copies(s):
                    copy.wait() if finish else copy.start()


def put_half(half, info, parts, whole):
    for t in range(RING):
        for s in range(RING):
            near = (info[1 - half] - s) % RING
            far = (info[half] - t) % RING
            at = pl.multiple_of(far * CHUNK + near * PIECE, PIECE)
            whole[pl.ds(at, PIECE), :] = parts[t][s]


SIDE = F // 3


def upper_blocks(left, right, out, turned=False):
    for j in range(3):
        rows, cols = slice(0, (j + 1) * SIDE), slice(j * SIDE, (j + 1) * SIDE)
        if turned:
            out[rows, cols] = lax.dot_general(
                left[rows, :], right[cols, :], (((1,), (1,)), ((), ())), preferred_element_type=f32
            )
        else:
            out[rows, cols] = jnp.dot(left[rows, :], right[:, cols], preferred_element_type=f32)


def mirror(out):
    for j in range(3):
        for i in range(j):
            low, high = slice(i * SIDE, (i + 1) * SIDE), slice(j * SIDE, (j + 1) * SIDE)
            out[high, low] = out[low, high].T


def gram_kernel(info, *rest):
    parts, (raw, first_half) = rest[:RING], rest[RING:]
    put_half(0, info, parts, first_half)
    upper_blocks(first_half, first_half, raw, True)


def sweep_kernel(info, raw_first, first_half, *rest):
    parts, kept, sent = rest[:RING], rest[RING], rest[RING + 1]
    second_half, half_gram, half_poly, turned, block, gram, other = rest[RING + 2 :]
    put_half(1, info, parts, second_half)
    upper_blocks(second_half, second_half, other, True)
    for j in range(3):
        rows, cols = slice(0, (j + 1) * SIDE), slice(j * SIDE, (j + 1) * SIDE)
        gram[rows, cols] = other[rows, cols] + raw_first[rows, cols]
    mirror(gram)
    diagonal = lax.broadcasted_iota(jnp.int32, (SIDE, SIDE), 0) == lax.broadcasted_iota(
        jnp.int32, (SIDE, SIDE), 1
    )
    trace = 0.0
    for j in range(3):
        one = slice(j * SIDE, (j + 1) * SIDE)
        trace = trace + jnp.sum(jnp.where(diagonal, gram[one, one], 0.0))
    inverse = 1.0 / (jnp.sqrt(trace) + norm_eps)
    gram[...] = gram[...] * inverse * inverse

    def poly_of():
        half_gram[...] = gram[...].astype(bf16)
        upper_blocks(half_gram, half_gram, other)
        mirror(other)
        return (ns_second * gram[...] + ns_third * other[...]).astype(bf16)

    half_poly[...] = poly_of()
    upper_blocks(half_poly, half_gram, other)
    mirror(other)
    gram[...] = ns_first * gram[...] + other[...]
    half_gram[...] = gram[...].astype(bf16)
    upper_blocks(half_gram, half_poly, other)
    mirror(other)
    gram[...] = ns_first * gram[...] + other[...]
    place = info[0] * RING + info[1]
    column = pl.multiple_of((place % (HALF // COLS)) * COLS, COLS)
    for half, ref in ((0, first_half), (1, second_half)):

        @pl.when(place // (HALF // COLS) == half)
        def _(ref=ref):
            block[...] = ref[:, pl.ds(column, COLS)]

    mine = block[...]
    first = inverse * (
        ns_first * mine.astype(f32) + jnp.dot(half_poly[...], mine, preferred_element_type=f32)
    )
    first = first.astype(bf16)
    last = poly_of()
    newer = ns_first * first.astype(f32) + jnp.dot(last, first, preferred_element_type=f32)
    turned[...] = (jnp.sqrt(jnp.float32(D)) * newer).T
    width = COLS // 2
    for ref, core in ((kept, info[2]), (sent, 1 - info[2])):
        ref[...] = turned[pl.ds(pl.multiple_of(core * width, width), width), :].astype(bf16)


def out_shapes(count):
    return [jax.ShapeDtypeStruct((count, CHUNK, HALF), bf16)] * 8


def call(kernel, flops, room, out_shape, scratch, scalars, operands, far=0, out_far=False):
    several = isinstance(out_shape, list)
    operands = [
        pltpu.with_memory_space_constraint(v, pltpu.HBM) if i < far else v
        for i, v in enumerate(operands)
    ]
    specs = [pl.BlockSpec(memory_space=pltpu.HBM)] * far
    specs += [pl.BlockSpec(memory_space=pltpu.VMEM)] * (len(operands) - far)
    out_spec = pl.BlockSpec(memory_space=pltpu.HBM if out_far else pltpu.VMEM)
    return pl.pallas_call(
        kernel,
        in_specs=[pl.BlockSpec(memory_space=pltpu.SMEM)] * len(scalars) + specs,
        out_specs=[out_spec] * len(out_shape) if several else out_spec,
        out_shape=out_shape,
        scratch_shapes=scratch,
        compiler_params=pltpu.CompilerParams(vmem_limit_bytes=room * 1024 * 1024),
        cost_estimate=pl.CostEstimate(flops=flops, bytes_accessed=flops // 500, transcendentals=0),
    )(*scalars, *operands)


AXES = ("dp_0", "dp_1")


def gather_stage(values, flip):
    found = [[values[0]], [values[1]]]
    received = {}
    for s in SHIFTS:
        for half in range(2):
            axis = AXES[1 - half] if flip else AXES[half]
            received[half, s] = shift(values[half], axis, s)
    for half in range(2):
        found[half] += [received[half, s] for s in range(1, RING)]
    return found


def per_device(token_inputs, cotangent, gate, up, down_weight, block_expert, block_count):
    z, x, c, y = (lax.axis_index(a) for a in DP_REP)
    rows = BLK * BLOCK
    turned = jnp.swapaxes(down_weight, 1, 2)
    other = swap(turned)
    own = lax.dynamic_index_in_dim(turned, c, 0, False)
    info = jnp.stack([z, x, c, y]).astype(jnp.int32)
    columns = call(
        turn_kernel,
        F * D,
        4,
        [jax.ShapeDtypeStruct((F // 2, COLS), bf16)] * 2,
        [pltpu.VMEM((COLS, F), f32)],
        [info],
        [own, other],
    )
    count_b, expert_b = swap(block_count), swap(block_expert)
    columns, gate, up, cotangent, token_inputs, count_b, expert_b = lax.optimization_barrier(
        (columns, gate, up, cotangent, token_inputs, count_b, expert_b)
    )
    stage = gather_stage(columns, False)
    stacked = [jnp.stack(v) for v in stage]
    stage = gather_stage(stacked, True)
    weights = stage[0] + stage[1]

    gate_b, up_b = swap(gate), swap(up)
    cot_b, tok_b = swap(cotangent), swap(token_inputs)

    factor_shape = jax.ShapeDtypeStruct((F, 2 * rows), bf16)
    *hidden_out, for_gate, for_up = call(
        hidden_kernel,
        2 * F * 2 * rows * D,
        12,
        out_shapes(1) + [factor_shape] * 2,
        [
            pltpu.VMEM((rows, F), bf16),
            pltpu.VMEM((rows, F), bf16),
            pltpu.VMEM((rows, D), bf16),
            pltpu.VMEM((F, 2 * rows), bf16),
            pltpu.VMEM((F, TILE), f32),
            pltpu.SemaphoreType.DMA((3,)),
        ],
        [info, block_count, block_expert, count_b, expert_b],
        [gate, up, cotangent, gate_b, up_b, cot_b],
        3,
    )
    grads_out = call(
        grads_kernel,
        6 * F * 2 * rows * D,
        18,
        out_shapes(2),
        [
            pltpu.VMEM((rows, D), bf16),
            pltpu.VMEM((rows, D), bf16),
            pltpu.VMEM((F, D), bf16),
            pltpu.VMEM((2 * F, 2 * rows), bf16),
            pltpu.VMEM((F, TILE), f32),
            pltpu.SemaphoreType.DMA((2,)),
        ],
        [info],
        [cotangent, token_inputs, for_gate, for_up, cot_b, tok_b, *weights],
        2,
    )

    def exchanged(parts, axes):
        got = {}
        for s in SHIFTS:
            for half in range(2):
                got[half, s] = shift(parts[half][s], axes[half], s)
        return [[parts[half][0]] + [got[half, s] for s in SHIFTS] for half in range(2)]

    hidden_terms = exchanged([hidden_out[:RING], hidden_out[RING:]], AXES)
    grads_terms = exchanged([grads_out[:RING], grads_out[RING:]], AXES)

    def fold(half):
        return call(
            functools.partial(fold_kernel, half),
            F * HALF * RING,
            4,
            [jax.ShapeDtypeStruct((3, PIECE, HALF), bf16)] * 4,
            [],
            [info],
            [*grads_terms[half], *hidden_terms[half]],
        )

    second = [fold(half) for half in range(2)]
    final_terms = exchanged(second, AXES[::-1])
    blocks = (2, PIECE, HALF)
    parts = call(
        finish_kernel,
        F * D,
        4,
        [jax.ShapeDtypeStruct(blocks, bf16)] * RING,
        [],
        [info],
        [*final_terms[0], *final_terms[1]],
    )
    arrived = [shift(parts[s], "rep", s) for s in SHIFTS]
    block = call(
        settle_kernel,
        F * D,
        4,
        [jax.ShapeDtypeStruct((PIECE, HALF), bf16)] * 2,
        [],
        [info],
        [parts[0], *arrived],
    )
    stage = gather_stage(block, True)
    stage = gather_stage([jnp.stack(v) for v in stage], False)
    raw, first_half = call(
        gram_kernel,
        F * F * D,
        8,
        [jax.ShapeDtypeStruct((F, F), f32), jax.ShapeDtypeStruct((F, HALF), bf16)],
        [],
        [info],
        stage[0],
    )
    kept, sent = call(
        sweep_kernel,
        8 * F * F * F,
        26,
        [jax.ShapeDtypeStruct((COLS // 2, F), bf16)] * 2,
        [
            pltpu.VMEM((F, HALF), bf16),
            pltpu.VMEM((F, F), bf16),
            pltpu.VMEM((F, F), bf16),
            pltpu.VMEM((COLS, F), f32),
            pltpu.VMEM((F, COLS), bf16),
            pltpu.VMEM((F, F), f32),
            pltpu.VMEM((F, F), f32),
        ],
        [info],
        [raw, first_half, *stage[1]],
    )
    narrow = (2, COLS // 2, F)
    pair = call(
        pair_kernel, F * COLS, 2, jax.ShapeDtypeStruct(narrow, bf16), [], [info], [kept, swap(sent)]
    )
    pieces = {0: pair, **{s: shift(pair, "rep", s) for s in SHIFTS}}
    everyone = call(
        spread_kernel,
        F * COLS,
        4,
        jax.ShapeDtypeStruct((2, 3, COLS // 2, F), bf16),
        [pltpu.SemaphoreType.DMA((RING, 2))],
        [info],
        [pieces[s] for s in range(RING)],
        out_far=True,
    )
    return jnp.swapaxes(everyone, 2, 3)


def solution(mesh):
    torus = Mesh(mesh.devices.reshape(4, 4, 2, mesh.shape["rep"]), DP_REP)

    return jax.shard_map(
        per_device,
        mesh=torus,
        in_specs=(
            P(DP_REP, None),
            P(DP_REP, None),
            P(DP_REP, None),
            P(DP_REP, None),
            P(None, None, DP),
            P(DP_REP),
            P(DP_REP),
        ),
        out_specs=P(None, None, None, DP),
        check_vma=False,
    )
```

```python
import functools

import jax
import jax.numpy as jnp
from jax import lax
from jax.experimental import pallas as pl
from jax.experimental.pallas import tpu as pltpu
from jax.sharding import Mesh
from jax.sharding import PartitionSpec as P


DP = ("dp_0", "dp_1", "dp_2")
DP_REP = ("dp_0", "dp_1", "dp_2", "rep")

ns_first = 3.4445
ns_second = -4.775
ns_third = 2.0315
norm_eps = 1e-07

F = 768
D = 2048
BLOCK = 128
BLK = 4
HALF = D // 2
TILE = 512
RING = 4
CHUNK = F // RING
PIECE = CHUNK // RING
COLS = D // 16
SHIFTS = (1, 3, 2)
f32 = jnp.float32
bf16 = jnp.bfloat16


def shift(value, axis, by):
    return lax.ppermute(value, axis, [(i, (i + by) % RING) for i in range(RING)])


def swap(value):
    return lax.ppermute(value, "dp_2", [(0, 1), (1, 0)])


def turn_kernel(info, own, other, first, second, rows):
    width = COLS // 2
    here = info[2]
    rows[pl.ds(pl.multiple_of(here * width, width), width), :] = own[...].astype(f32)
    rows[pl.ds(pl.multiple_of((1 - here) * width, width), width), :] = other[here].astype(f32)
    value = rows[...].T.astype(bf16)
    first[...] = value[: F // 2]
    second[...] = value[F // 2 :]


def finish_kernel(info, *rest):
    terms, outs = rest[:8], rest[8:]
    for s in range(RING):
        matrix = (info[3] + s) % RING
        at = jnp.minimum(matrix, 2)
        for half in range(2):
            value = terms[half * RING][at].astype(f32)
            for j in range(1, RING):
                value = value + terms[half * RING + j][at].astype(f32)
            outs[s][half] = jnp.where(matrix < 3, value, 0.0).astype(bf16)


def products(half, place, left, right_a, right_b, acc, outs):
    rows = BLK * BLOCK
    mats = left.shape[0] // F

    def tile(n, carry):
        to = pl.ds(pl.multiple_of(n * TILE, TILE), TILE)
        at = pl.ds(pl.multiple_of(half * HALF + n * TILE, TILE), TILE)
        for m in range(mats):
            one = pl.ds(m * F, F)
            acc[...] = jnp.dot(
                left[one, :rows], right_a[:, at], preferred_element_type=f32
            ) + jnp.dot(left[one, rows:], right_b[:, at], preferred_element_type=f32)
            for s in range(RING):
                chunk = (place + s) % RING
                value = acc[pl.ds(pl.multiple_of(chunk * CHUNK, CHUNK), CHUNK), :]
                outs[half * RING + s][m, :, to] = value.astype(bf16)
        return carry

    lax.fori_loop(0, HALF // TILE, tile, 0)


def hidden_kernel(info, count_a, expert_a, count_b, expert_b, gate_h, up_h, cot_h, *rest):
    gate_b, up_b, cot_b = rest[:3]
    outs, for_gate, for_up = rest[3:11], rest[11], rest[12]
    gate_a, up_a, cot_a, left, acc, sems = rest[13:]
    copies = [
        pltpu.make_async_copy(source, target, sems.at[i])
        for i, (source, target) in enumerate(((gate_h, gate_a), (up_h, up_a), (cot_h, cot_a)))
    ]
    for copy in copies:
        copy.start()

    def factors(gate_ref, up_ref, count, expert, base):
        def block(i, carry):
            rows = pl.ds(pl.multiple_of(i * BLOCK, BLOCK), BLOCK)
            gate = gate_ref[rows, :].T.astype(f32)
            up = up_ref[rows, :].T.astype(f32)
            limit = jnp.where(expert[i] == info[2], count[i], 0)
            live = lax.broadcasted_iota(jnp.int32, (F, BLOCK), 1) < limit
            sig = jax.nn.sigmoid(gate)
            to = pl.ds(pl.multiple_of(base + i * BLOCK, BLOCK), BLOCK)
            common = jnp.where(live, sig, 0.0)
            factor = common * gate
            left[:, to] = (factor * up).astype(bf16)
            for_up[:, to] = factor.astype(bf16)
            for_gate[:, to] = (common * up * (1.0 + gate * (1.0 - sig))).astype(bf16)
            return carry

        lax.fori_loop(0, BLK, block, 0)

    factors(gate_b, up_b, count_b, expert_b, BLK * BLOCK)
    copies[0].wait()
    copies[1].wait()
    factors(gate_a, up_a, count_a, expert_a, 0)
    copies[2].wait()
    for half in range(2):
        products(half, info[half], left, cot_a, cot_b, acc, outs)


def grads_kernel(info, cot_h, tok_h, for_gate, for_up, cot_b, tok_b, *rest):
    weights, outs, (cot_a, tok_a, whole, left, acc, sems) = rest[:8], rest[8:16], rest[16:]
    rows = BLK * BLOCK
    part = rows
    halves = F // 2
    copies = [
        pltpu.make_async_copy(source, target, sems.at[i])
        for i, (source, target) in enumerate(((cot_h, cot_a), (tok_h, tok_a)))
    ]
    for copy in copies:
        copy.start()
    for half in range(2):
        for t in range(RING):
            for s in range(RING):
                near = (info[half] - s) % RING
                far = (info[1 - half] - t) % RING
                z, x = (near, far) if half == 0 else (far, near)
                at = pl.multiple_of((z * RING + x) * COLS, COLS)
                whole[half * halves : (half + 1) * halves, pl.ds(at, COLS)] = weights[
                    half * RING + t
                ][s]

    def backward(cot, base):
        def step(i, carry):
            here = pl.ds(pl.multiple_of(i * part, part), part)
            to = pl.ds(pl.multiple_of(base + i * part, part), part)
            back = lax.dot_general(
                whole[...], cot[here, :], (((1,), (1,)), ((), ())), preferred_element_type=f32
            )
            left[:F, to] = (back * for_gate[:, to].astype(f32)).astype(bf16)
            left[F:, to] = (back * for_up[:, to].astype(f32)).astype(bf16)
            return carry

        lax.fori_loop(0, rows // part, step, 0)

    backward(cot_b, rows)
    copies[0].wait()
    backward(cot_a, 0)
    copies[1].wait()
    for half in range(2):
        products(half, info[half], left, tok_a, tok_b, acc, outs)


def fold_kernel(half, info, *rest):
    grads, hidden, outs = rest[:4], rest[4:8], rest[8:]
    place = info[1 - half]

    def total(terms, at):
        value = terms[0][:, at, :].astype(f32)
        for term in terms[1:]:
            value = value + term[:, at, :].astype(f32)
        return value.astype(bf16)

    for s in range(RING):
        at = pl.ds(pl.multiple_of(((place + s) % RING) * PIECE, PIECE), PIECE)
        outs[s][:2] = total(grads, at)
        outs[s][2:] = total(hidden, at)


def settle_kernel(info, *rest):
    terms, outs = rest[:RING], rest[RING:]
    for half in range(2):
        value = terms[0][half].astype(f32)
        for term in terms[1:]:
            value = value + term[half].astype(f32)
        outs[half][...] = value.astype(bf16)


def pair_kernel(info, kept, arrived, out):
    out[info[2]] = kept[...]
    out[1 - info[2]] = arrived[...]


def spread_kernel(info, *rest):
    pieces, out, sems = rest[:RING], rest[RING], rest[RING + 1]

    def copies(s):
        matrix = jnp.minimum((info[3] - s) % RING, 2)
        return [
            pltpu.make_async_copy(pieces[s].at[e], out.at[e, matrix], sems.at[s, e])
            for e in range(2)
        ]

    for finish in (False, True):
        for s in range(RING):

            @pl.when((info[3] - s) % RING < 3)
            def _(s=s, finish=finish):
                for copy in copies(s):
                    copy.wait() if finish else copy.start()


def put_half(half, info, parts, whole):
    for t in range(RING):
        for s in range(RING):
            near = (info[1 - half] - s) % RING
            far = (info[half] - t) % RING
            at = pl.multiple_of(far * CHUNK + near * PIECE, PIECE)
            whole[pl.ds(at, PIECE), :] = parts[t][s]


SIDE = F // 3


def upper_blocks(left, right, out, turned=False):
    for j in range(3):
        rows, cols = slice(0, (j + 1) * SIDE), slice(j * SIDE, (j + 1) * SIDE)
        if turned:
            out[rows, cols] = lax.dot_general(
                left[rows, :], right[cols, :], (((1,), (1,)), ((), ())), preferred_element_type=f32
            )
        else:
            out[rows, cols] = jnp.dot(left[rows, :], right[:, cols], preferred_element_type=f32)


def mirror(out):
    for j in range(3):
        for i in range(j):
            low, high = slice(i * SIDE, (i + 1) * SIDE), slice(j * SIDE, (j + 1) * SIDE)
            out[high, low] = out[low, high].T


def gram_kernel(info, *rest):
    parts, (raw, first_half) = rest[:RING], rest[RING:]
    put_half(0, info, parts, first_half)
    upper_blocks(first_half, first_half, raw, True)


def sweep_kernel(info, raw_first, first_half, *rest):
    parts, kept, sent = rest[:RING], rest[RING], rest[RING + 1]
    second_half, half_gram, half_poly, turned, block, gram, other = rest[RING + 2 :]
    put_half(1, info, parts, second_half)
    upper_blocks(second_half, second_half, other, True)
    for j in range(3):
        rows, cols = slice(0, (j + 1) * SIDE), slice(j * SIDE, (j + 1) * SIDE)
        gram[rows, cols] = other[rows, cols] + raw_first[rows, cols]
    mirror(gram)
    diagonal = lax.broadcasted_iota(jnp.int32, (SIDE, SIDE), 0) == lax.broadcasted_iota(
        jnp.int32, (SIDE, SIDE), 1
    )
    trace = 0.0
    for j in range(3):
        one = slice(j * SIDE, (j + 1) * SIDE)
        trace = trace + jnp.sum(jnp.where(diagonal, gram[one, one], 0.0))
    inverse = 1.0 / (jnp.sqrt(trace) + norm_eps)
    gram[...] = gram[...] * inverse * inverse

    def poly_of():
        half_gram[...] = gram[...].astype(bf16)
        upper_blocks(half_gram, half_gram, other)
        mirror(other)
        return (ns_second * gram[...] + ns_third * other[...]).astype(bf16)

    half_poly[...] = poly_of()
    upper_blocks(half_poly, half_gram, other)
    mirror(other)
    gram[...] = ns_first * gram[...] + other[...]
    half_gram[...] = gram[...].astype(bf16)
    upper_blocks(half_gram, half_poly, other)
    mirror(other)
    gram[...] = ns_first * gram[...] + other[...]
    place = info[0] * RING + info[1]
    column = pl.multiple_of((place % (HALF // COLS)) * COLS, COLS)
    for half, ref in ((0, first_half), (1, second_half)):

        @pl.when(place // (HALF // COLS) == half)
        def _(ref=ref):
            block[...] = ref[:, pl.ds(column, COLS)]

    mine = block[...]
    first = inverse * (
        ns_first * mine.astype(f32) + jnp.dot(half_poly[...], mine, preferred_element_type=f32)
    )
    first = first.astype(bf16)
    last = poly_of()
    newer = ns_first * first.astype(f32) + jnp.dot(last, first, preferred_element_type=f32)
    turned[...] = (jnp.sqrt(jnp.float32(D)) * newer).T
    width = COLS // 2
    for ref, core in ((kept, info[2]), (sent, 1 - info[2])):
        ref[...] = turned[pl.ds(pl.multiple_of(core * width, width), width), :].astype(bf16)


def out_shapes(count):
    return [jax.ShapeDtypeStruct((count, CHUNK, HALF), bf16)] * 8


def call(kernel, flops, room, out_shape, scratch, scalars, operands, far=0, out_far=False):
    several = isinstance(out_shape, list)
    operands = [
        pltpu.with_memory_space_constraint(v, pltpu.HBM) if i < far else v
        for i, v in enumerate(operands)
    ]
    specs = [pl.BlockSpec(memory_space=pltpu.HBM)] * far
    specs += [pl.BlockSpec(memory_space=pltpu.VMEM)] * (len(operands) - far)
    out_spec = pl.BlockSpec(memory_space=pltpu.HBM if out_far else pltpu.VMEM)
    return pl.pallas_call(
        kernel,
        in_specs=[pl.BlockSpec(memory_space=pltpu.SMEM)] * len(scalars) + specs,
        out_specs=[out_spec] * len(out_shape) if several else out_spec,
        out_shape=out_shape,
        scratch_shapes=scratch,
        compiler_params=pltpu.CompilerParams(vmem_limit_bytes=room * 1024 * 1024),
        cost_estimate=pl.CostEstimate(flops=flops, bytes_accessed=flops // 500, transcendentals=0),
    )(*scalars, *operands)


AXES = ("dp_0", "dp_1")


def gather_stage(values, flip):
    found = [[values[0]], [values[1]]]
    received = {}
    for s in SHIFTS:
        for half in range(2):
            axis = AXES[1 - half] if flip else AXES[half]
            received[half, s] = shift(values[half], axis, s)
    for half in range(2):
        found[half] += [received[half, s] for s in range(1, RING)]
    return found


def per_device(token_inputs, cotangent, gate, up, down_weight, block_expert, block_count):
    z, x, c, y = (lax.axis_index(a) for a in DP_REP)
    rows = BLK * BLOCK
    turned = jnp.swapaxes(down_weight, 1, 2)
    other = swap(turned)
    own = lax.dynamic_index_in_dim(turned, c, 0, False)
    info = jnp.stack([z, x, c, y]).astype(jnp.int32)
    columns = call(
        turn_kernel,
        F * D,
        4,
        [jax.ShapeDtypeStruct((F // 2, COLS), bf16)] * 2,
        [pltpu.VMEM((COLS, F), f32)],
        [info],
        [own, other],
    )
    count_b, expert_b = swap(block_count), swap(block_expert)
    columns, gate, up, cotangent, token_inputs, count_b, expert_b = lax.optimization_barrier(
        (columns, gate, up, cotangent, token_inputs, count_b, expert_b)
    )
    stage = gather_stage(columns, False)
    stacked = [jnp.stack(v) for v in stage]
    stage = gather_stage(stacked, True)
    weights = stage[0] + stage[1]

    gate_b, up_b = swap(gate), swap(up)
    cot_b, tok_b = swap(cotangent), swap(token_inputs)

    factor_shape = jax.ShapeDtypeStruct((F, 2 * rows), bf16)
    *hidden_out, for_gate, for_up = call(
        hidden_kernel,
        2 * F * 2 * rows * D,
        12,
        out_shapes(1) + [factor_shape] * 2,
        [
            pltpu.VMEM((rows, F), bf16),
            pltpu.VMEM((rows, F), bf16),
            pltpu.VMEM((rows, D), bf16),
            pltpu.VMEM((F, 2 * rows), bf16),
            pltpu.VMEM((F, TILE), f32),
            pltpu.SemaphoreType.DMA((3,)),
        ],
        [info, block_count, block_expert, count_b, expert_b],
        [gate, up, cotangent, gate_b, up_b, cot_b],
        3,
    )
    grads_out = call(
        grads_kernel,
        6 * F * 2 * rows * D,
        18,
        out_shapes(2),
        [
            pltpu.VMEM((rows, D), bf16),
            pltpu.VMEM((rows, D), bf16),
            pltpu.VMEM((F, D), bf16),
            pltpu.VMEM((2 * F, 2 * rows), bf16),
            pltpu.VMEM((F, TILE), f32),
            pltpu.SemaphoreType.DMA((2,)),
        ],
        [info],
        [cotangent, token_inputs, for_gate, for_up, cot_b, tok_b, *weights],
        2,
    )

    def exchanged(parts, axes):
        got = {}
        for s in SHIFTS:
            for half in range(2):
                got[half, s] = shift(parts[half][s], axes[half], s)
        return [[parts[half][0]] + [got[half, s] for s in SHIFTS] for half in range(2)]

    hidden_terms = exchanged([hidden_out[:RING], hidden_out[RING:]], AXES)
    grads_terms = exchanged([grads_out[:RING], grads_out[RING:]], AXES)

    def fold(half):
        return call(
            functools.partial(fold_kernel, half),
            F * HALF * RING,
            4,
            [jax.ShapeDtypeStruct((3, PIECE, HALF), bf16)] * 4,
            [],
            [info],
            [*grads_terms[half], *hidden_terms[half]],
        )

    second = [fold(half) for half in range(2)]
    final_terms = exchanged(second, AXES[::-1])
    blocks = (2, PIECE, HALF)
    parts = call(
        finish_kernel,
        F * D,
        4,
        [jax.ShapeDtypeStruct(blocks, bf16)] * RING,
        [],
        [info],
        [*final_terms[0], *final_terms[1]],
    )
    arrived = [shift(parts[s], "rep", s) for s in SHIFTS]
    block = call(
        settle_kernel,
        F * D,
        4,
        [jax.ShapeDtypeStruct((PIECE, HALF), bf16)] * 2,
        [],
        [info],
        [parts[0], *arrived],
    )
    stage = gather_stage(block, True)
    stage = gather_stage([jnp.stack(v) for v in stage], False)
    raw, first_half = call(
        gram_kernel,
        F * F * D,
        8,
        [jax.ShapeDtypeStruct((F, F), f32), jax.ShapeDtypeStruct((F, HALF), bf16)],
        [],
        [info],
        stage[0],
    )
    kept, sent = call(
        sweep_kernel,
        8 * F * F * F,
        26,
        [jax.ShapeDtypeStruct((COLS // 2, F), bf16)] * 2,
        [
            pltpu.VMEM((F, HALF), bf16),
            pltpu.VMEM((F, F), bf16),
            pltpu.VMEM((F, F), bf16),
            pltpu.VMEM((COLS, F), f32),
            pltpu.VMEM((F, COLS), bf16),
            pltpu.VMEM((F, F), f32),
            pltpu.VMEM((F, F), f32),
        ],
        [info],
        [raw, first_half, *stage[1]],
    )
    narrow = (2, COLS // 2, F)
    pair = call(
        pair_kernel, F * COLS, 2, jax.ShapeDtypeStruct(narrow, bf16), [], [info], [kept, swap(sent)]
    )
    pieces = {0: pair, **{s: shift(pair, "rep", s) for s in SHIFTS}}
    everyone = call(
        spread_kernel,
        F * COLS,
        4,
        jax.ShapeDtypeStruct((2, 3, COLS // 2, F), bf16),
        [pltpu.SemaphoreType.DMA((RING, 2))],
        [info],
        [pieces[s] for s in range(RING)],
        out_far=True,
    )
    return jnp.swapaxes(everyone, 2, 3)


def solution(mesh):
    torus = Mesh(mesh.devices.reshape(4, 4, 2, mesh.shape["rep"]), DP_REP)

    return jax.shard_map(
        per_device,
        mesh=torus,
        in_specs=(
            P(DP_REP, None),
            P(DP_REP, None),
            P(DP_REP, None),
            P(DP_REP, None),
            P(None, None, DP),
            P(DP_REP),
            P(DP_REP),
        ),
        out_specs=P(None, None, None, DP),
        check_vma=False,
    )
```
